32 devices in a mesh: members: 2 (over x), row: 16 (over z, y, core).
Axes of the slice: x: 2, y: 2, z: 4, core: 2. Of those that a mesh axis runs over, the one named last changes fastest.
Arguments:
- base: float32 [2, 3, 32, 384, 256], P(None, None, ('members', 'row')), parts along dimension 2, may hold values from -6 to 6
- section: float32 [2, 3, 32, 384, 256], P(None, None, ('members', 'row')), parts along dimension 2, may hold values from -12 to 12
- accum: float32 [2, 3, 32, 384, 256], P(None, None, ('members', 'row')), parts along dimension 2, may hold values from -6 to 6
- cutoffs: int32 [6], P('members'), parts along dimension 0, may hold values from 5 to 170, as said below
- force_waves: int32 [64, 3], P(('members', 'row')), parts along dimension 0, may hold values from -8 to 8, as said below
- force_phase: int32 [64], P(('members', 'row')), parts along dimension 0, may hold values from 0 to 255
- force_dir: float32 [64, 3], P(('members', 'row')), parts along dimension 0, may hold values from -12 to 12
Outputs:
- next_section: float32 [2, 3, 32, 384, 256], P(None, None, ('members', 'row')), parts along dimension 2
- accum_out: float32 [2, 3, 32, 384, 256], P(None, None, ('members', 'row')), parts along dimension 2
The draws below stay inside these ranges and needn't reach their ends.
There are 2 independent parts, one for each index of `members`. The reference program is written for one: setup_inputs(seed, part) draws one part's arguments, and reference() takes and returns one part's arrays. A program takes and returns all parts, laid end to end along the dimension named above; each array names one. Nothing has to cross between parts.
Inputs may be any that keep to these rules, and one draw needn't show every extreme that they name: cutoffs[0] lies in 128 to 170, cutoffs[1] in 128 to 170, cutoffs[2] in 5 to 6. `force_waves`: each row is (first, second, third) signed wavenumbers: the first within -8 to 8, the second within 0 to 8, the third within -3 to 3.
All inputs are finite; a program needn't handle non-finite values.
Results may differ from the reference program's by a relative error of at most 0.00005.
Values sent between devices are 32-bit elements; how exact they have to be, the bound alone decides.
A program may use at most 128 MiB of HBM per device.

```python
import math
import jax
import jax.numpy as jnp

NX = 512
NY = 512
PH = 256
KZ = 16
NZ = 20
KX = 384
KY = 256
NF = 32


def draw_cutoffs(key, part):
    subkeys = jax.random.split(jax.random.fold_in(key, 17), 3)
    cut_first = jax.random.randint(subkeys[0], (1,), NX // 4, NX // 3 + 1, dtype=jnp.int32)
    cut_second = jax.random.randint(subkeys[1], (1,), NY // 4, NY // 3 + 1, dtype=jnp.int32)
    cut_third = jax.random.randint(subkeys[2], (1,), NZ // 4, NZ // 3 + 1, dtype=jnp.int32)
    return jnp.concatenate([cut_first, cut_second, cut_third])


def draw_force_waves(key, part):
    subkeys = jax.random.split(jax.random.fold_in(key, 29), 3)
    along_first = jax.random.randint(subkeys[0], (NF, 1), -8, 9, dtype=jnp.int32)
    along_second = jax.random.randint(subkeys[1], (NF, 1), 0, 9, dtype=jnp.int32)
    along_third = jax.random.randint(subkeys[2], (NF, 1), -3, 4, dtype=jnp.int32)
    return jnp.concatenate([along_first, along_second, along_third], axis=1)


def touch_ends(values, own_key, least, high):
    longest = values.shape.index(max(values.shape))
    spots = []
    for shift in (0, 1):
        where = [jax.random.randint(jax.random.fold_in(own_key, axis), (), 0, length) for axis, length in enumerate(values.shape)]
        where[longest] = (where[longest] + shift) % values.shape[longest]
        spots.append(tuple(where))
    return values.at[spots[0]].set(least).at[spots[1]].set(high)


def levels(own_key, shape, cuts, least, largest):
    level, own = 1.0, jax.random.fold_in(own_key, 6)
    for axis_at, blocks in cuts:
        heights = jnp.exp(jax.random.uniform(jax.random.fold_in(own, axis_at), (blocks,), jnp.float32, least / len(cuts), largest / len(cuts)))
        level = level * jnp.repeat(heights, shape[axis_at] // blocks).reshape([-1 if axis == axis_at else 1 for axis in range(len(shape))])
    return level


def bell_draw(stream_key, shape, spread, bound, cuts=(), kind=jnp.bfloat16):
    result = jax.random.normal(stream_key, shape, jnp.float32) * spread
    if len(cuts) > 0:
        result = levels(stream_key, shape, cuts, -0.22, 0.18) * result
    return jnp.clip(result, min=-bound, max=bound).astype(kind)


def setup_inputs(seed: int = 0, part: int = 0) -> dict:
    arg_keys = jax.random.split(jax.random.key(seed), 8)
    part_splits = jax.random.split(jax.random.fold_in(arg_keys[7], part), 8)
    return {
        "base": bell_draw(part_splits[0], (2, 3, KZ, KX, KY), 1.0, 6.0, ((2, 16),), jnp.float32),
        "section": bell_draw(part_splits[1], (2, 3, KZ, KX, KY), 2.0, 12.0, ((2, 16),), jnp.float32),
        "accum": bell_draw(part_splits[2], (2, 3, KZ, KX, KY), 1.0, 6.0, ((2, 16),), jnp.float32),
        "cutoffs": draw_cutoffs(jax.random.fold_in(jax.random.fold_in(arg_keys[7], part), 71), part),
        "force_waves": draw_force_waves(jax.random.fold_in(jax.random.fold_in(arg_keys[7], part), 71), part),
        "force_phase": touch_ends(jax.random.randint(part_splits[5], (NF,), 0, PH), jax.random.fold_in(part_splits[5], 1), 0, PH - 1).astype(jnp.int32),
        "force_dir": bell_draw(part_splits[6], (NF, 3), 2.0, 12.0, ((0, 16),), jnp.float32),
    }


VISCOSITY = 0.04
SECTION_WEIGHT = 0.2
ACCUM_WEIGHT = 0.4 / 3.0

def signed_modes(length):
    position = jnp.arange(length, dtype=jnp.int32)
    return jnp.where(position < length // 2, position, position - length)

def rotate_quarter(values):
    return jnp.stack([-values[1], values[0]])

def inverse_field(spectral, weights):
    half_count = KX // 2
    half_depth = KZ // 2
    coeffs = (spectral[0] + 1j * spectral[1]) * weights
    gap_first = jnp.zeros((KZ, NX - KX, KY), coeffs.dtype)
    coeffs = jnp.concatenate([coeffs[:, :half_count], gap_first, coeffs[:, half_count:]], axis=1)
    gap_second = jnp.zeros((KZ, NX, NY - KY), coeffs.dtype)
    coeffs = jnp.concatenate([coeffs, gap_second], axis=2)
    gap_third = jnp.zeros((NZ - KZ, NX, NY), coeffs.dtype)
    coeffs = jnp.concatenate([coeffs[:half_depth], gap_third, coeffs[half_depth:]], axis=0)
    return jnp.real(jnp.fft.ifftn(coeffs)) * math.sqrt(NX * NY * NZ)

def forward_field(physical):
    half_count = KX // 2
    half_depth = KZ // 2
    coeffs = jnp.fft.fftn(physical) / math.sqrt(NX * NY * NZ)
    coeffs = jnp.concatenate([coeffs[:half_depth], coeffs[NZ - half_depth:]], axis=0)
    coeffs = jnp.concatenate([coeffs[:, :half_count], coeffs[:, NX - half_count:]], axis=1)[:, :, :KY]
    return jnp.stack([jnp.real(coeffs), jnp.imag(coeffs)]).astype(jnp.float32)

def reference(base, section, accum, cutoffs, force_waves, force_phase, force_dir):
    modes_first = signed_modes(KX)
    modes_second = jnp.arange(KY, dtype=jnp.int32)
    modes_third = signed_modes(KZ)
    retained = ((jnp.abs(modes_third)[:, None, None] <= cutoffs[2]) & (jnp.abs(modes_first)[None, :, None] <= cutoffs[0]) & (modes_second[None, None, :] <= cutoffs[1])).astype(jnp.float32)
    masked = section * retained
    wave_first = 8.0 / NX * modes_first.astype(jnp.float32)[None, :, None]
    wave_second = 8.0 / NX * modes_second.astype(jnp.float32)[None, None, :]
    wave_third = 8.0 / NZ * modes_third.astype(jnp.float32)[:, None, None]
    speed_one = masked[:, 0]
    speed_two = masked[:, 1]
    speed_three = masked[:, 2]
    spin = [rotate_quarter(wave_second * speed_three - wave_third * speed_two), rotate_quarter(wave_third * speed_one - wave_first * speed_three), rotate_quarter(wave_first * speed_two - wave_second * speed_one)]
    weights = jnp.where(modes_second == 0, 1.0, 2.0).astype(jnp.float32)
    velocity = [inverse_field(masked[:, component], weights) for component in range(3)]
    vorticity = [inverse_field(rotation, weights) for rotation in spin]
    crossed = [velocity[1] * vorticity[2] - velocity[2] * vorticity[1], velocity[2] * vorticity[0] - velocity[0] * vorticity[2], velocity[0] * vorticity[1] - velocity[1] * vorticity[0]]
    crossed_hat = jnp.stack([forward_field(term) for term in crossed], axis=1)
    turning = 2.0 * math.pi / PH * force_phase.astype(jnp.float32)
    values = jnp.stack([force_dir.T * jnp.cos(turning)[None, :], force_dir.T * jnp.sin(turning)[None, :]])
    forced = jnp.zeros(section.shape, jnp.float32).at[:, :, jnp.mod(force_waves[:, 2], KZ), jnp.mod(force_waves[:, 0], KX), force_waves[:, 1]].add(values)
    driving = crossed_hat * retained + forced
    inner = wave_first * driving[:, 0] + wave_second * driving[:, 1] + wave_third * driving[:, 2]
    squared = wave_first * wave_first + wave_second * wave_second + wave_third * wave_third
    anchor = (modes_first[None, :, None] == 0) & (modes_second[None, None, :] == 0) & (modes_third[:, None, None] == 0)
    share = inner / jnp.where(anchor, 1.0, squared)
    projected = driving - jnp.stack([wave_first * share, wave_second * share, wave_third * share], axis=1)
    tendency = projected - VISCOSITY * squared * section
    return (base + SECTION_WEIGHT * tendency, accum + ACCUM_WEIGHT * tendency)
```

```python
import functools
import math

import jax
import jax.numpy as jnp
import numpy as np
from jax import lax
from jax.experimental import pallas as pl
from jax.experimental.pallas import tpu as pltpu
from jax.sharding import PartitionSpec as P

NX = 512
NY = 512
PH = 256


PRECISE = lax.Precision.HIGH
LANES = 128
HALF = 64
MEMORY = pltpu.VMEM
VISCOSITY = 0.04
SECTION_WEIGHT = 0.2
ACCUM_WEIGHT = 0.4 / 3.0


def signed_modes(length):
    position = np.arange(length, dtype=np.int32)
    return np.where(position < length // 2, position, position - length)


def angle_grid(leading, trailing, length):
    product = np.mod(leading[:, None].astype(np.int64) * trailing[None, :], length)
    return 2.0 * math.pi / length * product.astype(np.float64)


def complex_table(angles):
    cosine = np.cos(angles)
    sine = np.sin(angles)
    return np.stack(
        [np.stack([cosine, sine], axis=1), np.stack([-sine, cosine], axis=1)], axis=0
    )


def exchange_kernel(devices, source, target, send_sem, recv_sem, own_sem):
    me = lax.axis_index("row")
    barrier = pltpu.get_barrier_semaphore()
    for step in range(1, devices):
        pl.semaphore_signal(
            barrier,
            inc=1,
            device_id={"row": lax.rem(me + step, devices)},
            device_id_type=pl.DeviceIdType.MESH,
        )
    own = pltpu.make_async_copy(source.at[me], target.at[me], own_sem)
    own.start()
    pl.semaphore_wait(barrier, devices - 1)
    copies = []
    for step in range(1, devices):
        other = lax.rem(me + step, devices)
        copy = pltpu.make_async_remote_copy(
            src_ref=source.at[other],
            dst_ref=target.at[me],
            send_sem=send_sem.at[step],
            recv_sem=recv_sem.at[step],
            device_id={"row": other},
            device_id_type=pl.DeviceIdType.MESH,
        )
        copy.start()
        copies.append(copy)
    own.wait()
    for copy in copies:
        copy.wait()


def exchange(blocks, identity):
    devices = blocks.shape[0]
    shape = blocks.shape
    return pl.pallas_call(
        functools.partial(exchange_kernel, devices),
        out_shape=jax.ShapeDtypeStruct(shape, blocks.dtype),
        in_specs=[pl.BlockSpec(memory_space=MEMORY)],
        out_specs=pl.BlockSpec(memory_space=MEMORY),
        scratch_shapes=[
            pltpu.SemaphoreType.DMA((devices,)),
            pltpu.SemaphoreType.DMA((devices,)),
            pltpu.SemaphoreType.DMA,
        ],
        compiler_params=pltpu.CompilerParams(
            collective_id=identity, has_side_effects=True, vmem_limit_bytes=32 << 20
        ),
    )(blocks)


def rotate_quarter(values):
    return jnp.stack([-values[1], values[0]])


def on_device(base, section, accum, cutoffs, force_waves, force_phase, force_dir):
    devices = lax.axis_size("row")
    planes = section.shape[2]
    kept_first = section.shape[3]
    kept_second = section.shape[4]
    stored_planes = planes * devices
    depth_cells = 5 * stored_planes // 4
    slab_cells = NX // devices
    unitary = 1.0 / math.sqrt(NX * NY * depth_cells)
    first_plane = lax.axis_index("row") * planes
    modes_first = signed_modes(kept_first)
    modes_second = np.arange(kept_second, dtype=np.int32)
    modes_third = signed_modes(stored_planes)
    plane_index = first_plane + jnp.arange(planes, dtype=jnp.int32)
    third_local = jnp.where(
        plane_index < stored_planes // 2, plane_index, plane_index - stored_planes
    )
    retained = (
        (jnp.abs(third_local)[:, None, None] <= cutoffs[2])
        & (jnp.abs(modes_first)[None, :, None] <= cutoffs[0])
        & (modes_second[None, None, :] <= cutoffs[1])
    ).astype(jnp.float32)
    masked = section * retained
    first_scale = 8.0 / NX
    third_scale = 8.0 / depth_cells
    wave_first = first_scale * modes_first.astype(jnp.float32)[None, :, None]
    wave_second = first_scale * modes_second.astype(jnp.float32)[None, None, :]
    wave_third = third_scale * third_local.astype(jnp.float32)[:, None, None]
    packed = jnp.concatenate(
        [force_waves.astype(jnp.float32), force_phase.astype(jnp.float32)[:, None], force_dir], axis=1
    )
    gathered = lax.all_gather(packed, "row", axis=0, tiled=True)
    section_kept, gathered = lax.optimization_barrier((masked[:, :, :, :, : LANES + HALF], gathered))
    weights = np.where(modes_second == 0, 1.0, 2.0).astype(np.float32)
    section_kept = section_kept * weights[: LANES + HALF]
    upper = section_kept[..., LANES:]
    doubled = jnp.stack(
        [section_kept[..., :LANES], jnp.concatenate([upper, upper], axis=-1)], axis=2
    )
    fields = jnp.concatenate(
        [doubled, rotate_quarter(wave_first * doubled[:, 1:3])], axis=1
    )
    count = fields.shape[1]
    half_slab = slab_cells // 2
    rows = slab_cells + half_slab
    first_cells = np.arange(NX, dtype=np.int32)
    third_cells = np.arange(depth_cells, dtype=np.int32)
    second_cells = np.arange(NY, dtype=np.int32)
    table_first = (unitary * complex_table(angle_grid(modes_first, first_cells, NX))).astype(np.float32)
    table_third = complex_table(angle_grid(modes_third, third_cells, depth_cells)).astype(np.float32)
    second_angles = angle_grid(modes_second[: LANES + HALF], second_cells, NY)
    table_second = np.stack([np.cos(second_angles), -np.sin(second_angles)]).astype(np.float32)
    table_lower = table_second[:, :LANES]
    table_upper = np.zeros((2, 2, HALF, 2, NY), np.float32)
    table_upper[:, 0, :, 0] = table_second[:, LANES:]
    table_upper[:, 1, :, 1] = table_second[:, LANES:]
    table_upper = table_upper.reshape(2, LANES, 2, NY)
    third_waves = (third_scale * modes_third.astype(np.float32))[:, None, None]
    column = first_scale * modes_second.astype(np.float32)
    column_waves = np.concatenate(
        [
            np.broadcast_to(column[:LANES], (slab_cells, LANES)),
            np.broadcast_to(np.tile(column[LANES : LANES + HALF], 2), (half_slab, LANES)),
        ]
    )
    spread = jnp.einsum("rfgkab,raqx->qfkgxb", fields, table_first, precision=PRECISE)
    spread = spread.reshape(2, count, planes, 2, devices, 2, half_slab, LANES)
    lower = spread[:, :, :, 0].reshape(2, count, planes, devices, slab_cells, LANES)
    lane = jnp.arange(LANES) < HALF
    higher = jnp.where(lane, spread[:, :, :, 1, :, 0], spread[:, :, :, 1, :, 1])
    blocks = jnp.concatenate([lower, higher], axis=4).transpose(3, 2, 0, 1, 4, 5)
    blocks = exchange(blocks, 0).reshape(stored_planes, 2, count, rows, LANES)
    parcel = blocks.transpose(1, 2, 0, 3, 4)
    speed_one = parcel[:, 0]
    speed_two = parcel[:, 1]
    speed_three = parcel[:, 2]
    slope_two = parcel[:, 3]
    slope_three = parcel[:, 4]
    spin = jnp.stack(
        [
            rotate_quarter(column_waves * speed_three - third_waves * speed_two),
            rotate_quarter(third_waves * speed_one) - slope_three,
            slope_two - rotate_quarter(column_waves * speed_one),
        ],
        axis=1,
    )
    parcel = jnp.concatenate([parcel[:, :3], spin], axis=1)
    along_third = jnp.einsum("rfcnb,rcqz->qfznb", parcel, table_third, precision=PRECISE)
    physical = jnp.einsum(
        "rfznb,rby->fzny", along_third[..., :slab_cells, :], table_lower, precision=PRECISE
    )
    physical = physical + jnp.einsum(
        "rfznb,rbhy->fzhny", along_third[..., slab_cells:, :], table_upper, precision=PRECISE
    ).reshape(physical.shape)
    velocity = physical[:3]
    vorticity = physical[3:]
    crossed = jnp.stack(
        [
            velocity[1] * vorticity[2] - velocity[2] * vorticity[1],
            velocity[2] * vorticity[0] - velocity[0] * vorticity[2],
            velocity[0] * vorticity[1] - velocity[1] * vorticity[0],
        ]
    )
    halves = crossed.reshape(3, depth_cells, 2, half_slab, NY)
    spectral_second = jnp.concatenate(
        [
            jnp.einsum("czny,rby->rcznb", crossed, table_lower, precision=PRECISE),
            jnp.einsum("czhny,rbhy->rcznb", halves, table_upper, precision=PRECISE),
        ],
        axis=3,
    )
    terms = jnp.einsum("rcznb,qkrz->kqcnb", spectral_second, table_third, precision=PRECISE)
    terms = terms.reshape(devices, planes, 2, 3, rows, LANES)
    pencils = exchange(terms, 1).transpose(2, 3, 1, 0, 4, 5)
    low = pencils[..., :slab_cells, :].reshape(2, 3, planes, NX, LANES)
    high = pencils[..., slab_cells:, :]
    table_split = table_first.reshape(2, kept_first, 2, devices, 2, half_slab)
    spectral_low = jnp.einsum("rfkxn,qarx->qfkan", low, table_first, precision=PRECISE)
    spectral_high = jnp.einsum(
        "rfkdnl,qardhn->hqfkal", high, table_split, precision=PRECISE
    )
    spectral_high = spectral_high[0, ..., :HALF] + spectral_high[1, ..., HALF:]
    spectral = jnp.concatenate([spectral_low, spectral_high], axis=-1)
    spectral = jnp.pad(spectral, [(0, 0)] * 4 + [(0, kept_second - LANES - HALF)])
    first_range = jnp.arange(kept_first, dtype=jnp.int32)
    second_range = jnp.arange(kept_second, dtype=jnp.int32)
    plane_range = jnp.arange(planes, dtype=jnp.int32)
    numbers = gathered[:, :3].astype(jnp.int32)
    phases = gathered[:, 3]
    directions = gathered[:, 4:7]
    column_hit = (jnp.mod(numbers[:, 0], kept_first)[:, None] == first_range[None, :]).astype(
        jnp.float32
    )
    second_hit = (numbers[:, 1][:, None] == second_range[None, :]).astype(jnp.float32)
    plane_hit = (
        (jnp.mod(numbers[:, 2], stored_planes) - first_plane)[:, None] == plane_range[None, :]
    ).astype(jnp.float32)
    turning = 2.0 * math.pi / PH * phases
    values = jnp.stack(
        [directions.T * jnp.cos(turning)[None, :], directions.T * jnp.sin(turning)[None, :]]
    )
    placed = (
        values[:, :, None, None, :]
        * plane_hit.T[None, None, :, None, :]
        * column_hit.T[None, None, None, :, :]
    )
    forced = jnp.einsum("rckan,nb->rckab", placed, second_hit, precision=PRECISE)
    driving = spectral * retained + forced
    inner = wave_first * driving[:, 0] + wave_second * driving[:, 1] + wave_third * driving[:, 2]
    squared = wave_first * wave_first + wave_second * wave_second + wave_third * wave_third
    anchor = (
        (modes_first[None, :, None] == 0)
        & (modes_second[None, None, :] == 0)
        & (third_local[:, None, None] == 0)
    )
    share = inner / jnp.where(anchor, 1.0, squared)
    projected = driving - jnp.stack(
        [wave_first * share, wave_second * share, wave_third * share], axis=1
    )
    tendency = projected - VISCOSITY * squared * section
    return (base + SECTION_WEIGHT * tendency, accum + ACCUM_WEIGHT * tendency)


def solution(mesh):
    placed = (
        P(None, None, ("members", "row"), None, None),
        P(None, None, ("members", "row"), None, None),
        P(None, None, ("members", "row"), None, None),
        P("members"),
        P(("members", "row"), None),
        P(("members", "row")),
        P(("members", "row"), None),
    )
    return jax.shard_map(
        on_device,
        mesh=mesh,
        in_specs=placed,
        out_specs=(
            P(None, None, ("members", "row"), None, None),
            P(None, None, ("members", "row"), None, None),
        ),
        check_vma=False,
    )
```

```python
import functools
import math

import jax
import jax.numpy as jnp
import numpy as np
from jax import lax
from jax.experimental import pallas as pl
from jax.experimental.pallas import tpu as pltpu
from jax.sharding import PartitionSpec as P

NX = 512
NY = 512
PH = 256


PRECISE = lax.Precision.HIGH
LANES = 128
HALF = 64
MEMORY = pltpu.VMEM
VISCOSITY = 0.04
SECTION_WEIGHT = 0.2
ACCUM_WEIGHT = 0.4 / 3.0


def signed_modes(length):
    position = np.arange(length, dtype=np.int32)
    return np.where(position < length // 2, position, position - length)


def angle_grid(leading, trailing, length):
    product = np.mod(leading[:, None].astype(np.int64) * trailing[None, :], length)
    return 2.0 * math.pi / length * product.astype(np.float64)


def complex_table(angles):
    cosine = np.cos(angles)
    sine = np.sin(angles)
    return np.stack(
        [np.stack([cosine, sine], axis=1), np.stack([-sine, cosine], axis=1)], axis=0
    )


def exchange_kernel(devices, alive, outward, *refs):
    if outward:
        source, extra, target, gathered, send_sem, recv_sem, own_sem, send_extra, recv_extra = refs
    else:
        source, target, send_sem, recv_sem, own_sem = refs
    me = lax.axis_index("row")

    def living(index):
        return (index <= alive) | (index >= devices - alive)

    barrier = pltpu.get_barrier_semaphore()
    for step in range(1, devices):
        pl.semaphore_signal(
            barrier,
            inc=1,
            device_id={"row": lax.rem(me + step, devices)},
            device_id_type=pl.DeviceIdType.MESH,
        )
    own = pltpu.make_async_copy(source.at[me], target.at[me], own_sem)
    mine = living(me)
    if outward:
        for index in range(alive + 1, devices - alive):
            target[index] = jnp.zeros(target.shape[1:], target.dtype)
        gathered[me] = extra[...]
    else:
        @pl.when(jnp.logical_not(mine))
        def _():
            for index in range(devices):
                target[index] = jnp.zeros(target.shape[1:], target.dtype)

    @pl.when(mine)
    def _():
        own.start()

    pl.semaphore_wait(barrier, devices - 1)
    copies = []
    for step in range(1, devices):
        other = lax.rem(me + step, devices)
        sender = lax.rem(me + devices - step, devices)
        sends, receives = (mine, living(sender)) if outward else (living(other), mine)
        copy = pltpu.make_async_remote_copy(
            src_ref=source.at[other],
            dst_ref=target.at[me],
            send_sem=send_sem.at[step],
            recv_sem=recv_sem.at[step],
            device_id={"row": other},
            device_id_type=pl.DeviceIdType.MESH,
        )
        small = None
        if outward:
            small = pltpu.make_async_remote_copy(
                src_ref=extra,
                dst_ref=gathered.at[me],
                send_sem=send_extra.at[step],
                recv_sem=recv_extra.at[step],
                device_id={"row": other},
                device_id_type=pl.DeviceIdType.MESH,
            )
            small.start()
        pl.when(sends)(copy.start)
        copies.append((copy, small, sends, receives))
    pl.when(mine)(own.wait)
    for copy, small, sends, receives in copies:
        pl.when(sends)(copy.wait_send)
        pl.when(receives)(copy.wait_recv)
        if outward:
            small.wait()


def exchange(blocks, identity, alive, extra=None):
    devices = blocks.shape[0]
    outward = extra is not None
    operands = (blocks, extra) if outward else (blocks,)
    shapes = [jax.ShapeDtypeStruct(blocks.shape, blocks.dtype)]
    sems = [
        pltpu.SemaphoreType.DMA((devices,)),
        pltpu.SemaphoreType.DMA((devices,)),
        pltpu.SemaphoreType.DMA,
    ]
    if outward:
        shapes.append(jax.ShapeDtypeStruct((devices,) + extra.shape, extra.dtype))
        sems += [pltpu.SemaphoreType.DMA((devices,)), pltpu.SemaphoreType.DMA((devices,))]
    return pl.pallas_call(
        functools.partial(exchange_kernel, devices, alive, outward),
        out_shape=shapes,
        in_specs=[pl.BlockSpec(memory_space=MEMORY)] * len(operands),
        out_specs=[pl.BlockSpec(memory_space=MEMORY)] * len(shapes),
        scratch_shapes=sems,
        compiler_params=pltpu.CompilerParams(
            collective_id=identity, has_side_effects=True, vmem_limit_bytes=32 << 20
        ),
    )(*operands)


def rotate_quarter(values):
    return jnp.stack([-values[1], values[0]])


def on_device(base, section, accum, cutoffs, force_waves, force_phase, force_dir):
    devices = lax.axis_size("row")
    planes = section.shape[2]
    kept_first = section.shape[3]
    kept_second = section.shape[4]
    stored_planes = planes * devices
    depth_cells = 5 * stored_planes // 4
    slab_cells = NX // devices
    unitary = 1.0 / math.sqrt(NX * NY * depth_cells)
    first_plane = lax.axis_index("row") * planes
    modes_first = signed_modes(kept_first)
    modes_second = np.arange(kept_second, dtype=np.int32)
    modes_third = signed_modes(stored_planes)
    plane_index = first_plane + jnp.arange(planes, dtype=jnp.int32)
    third_local = jnp.where(
        plane_index < stored_planes // 2, plane_index, plane_index - stored_planes
    )
    retained = (
        (jnp.abs(third_local)[:, None, None] <= cutoffs[2])
        & (jnp.abs(modes_first)[None, :, None] <= cutoffs[0])
        & (modes_second[None, None, :] <= cutoffs[1])
    ).astype(jnp.float32)
    masked = section * retained
    first_scale = 8.0 / NX
    third_scale = 8.0 / depth_cells
    wave_first = first_scale * modes_first.astype(jnp.float32)[None, :, None]
    wave_second = first_scale * modes_second.astype(jnp.float32)[None, None, :]
    wave_third = third_scale * third_local.astype(jnp.float32)[:, None, None]
    packed = jnp.concatenate(
        [force_waves.astype(jnp.float32), force_phase.astype(jnp.float32)[:, None], force_dir], axis=1
    )
    listed = packed.shape
    packed = jnp.pad(packed, [(0, -listed[0] % 8), (0, LANES - listed[1])])
    alive = depth_cells // 3 if planes == 1 else devices
    section_kept = masked[:, :, :, :, : LANES + HALF]
    weights = np.where(modes_second == 0, 1.0, 2.0).astype(np.float32)
    section_kept = section_kept * weights[: LANES + HALF]
    upper = section_kept[..., LANES:]
    doubled = jnp.stack(
        [section_kept[..., :LANES], jnp.concatenate([upper, upper], axis=-1)], axis=2
    )
    fields = jnp.concatenate(
        [doubled, rotate_quarter(wave_first * doubled[:, 1:3])], axis=1
    )
    count = fields.shape[1]
    half_slab = slab_cells // 2
    rows = slab_cells + half_slab
    first_cells = np.arange(NX, dtype=np.int32)
    third_cells = np.arange(depth_cells, dtype=np.int32)
    second_cells = np.arange(NY, dtype=np.int32)
    table_first = (unitary * complex_table(angle_grid(modes_first, first_cells, NX))).astype(np.float32)
    table_third = complex_table(angle_grid(modes_third, third_cells, depth_cells)).astype(np.float32)
    second_angles = angle_grid(modes_second[: LANES + HALF], second_cells, NY)
    table_second = np.stack([np.cos(second_angles), -np.sin(second_angles)]).astype(np.float32)
    table_lower = table_second[:, :LANES]
    table_upper = np.zeros((2, 2, HALF, 2, NY), np.float32)
    table_upper[:, 0, :, 0] = table_second[:, LANES:]
    table_upper[:, 1, :, 1] = table_second[:, LANES:]
    table_upper = table_upper.reshape(2, LANES, 2, NY)
    third_waves = (third_scale * modes_third.astype(np.float32))[:, None, None]
    column = first_scale * modes_second.astype(np.float32)
    column_waves = np.concatenate(
        [
            np.broadcast_to(column[:LANES], (slab_cells, LANES)),
            np.broadcast_to(np.tile(column[LANES : LANES + HALF], 2), (half_slab, LANES)),
        ]
    )
    spread = jnp.einsum("rfgkab,raqx->qfkgxb", fields, table_first, precision=PRECISE)
    spread = spread.reshape(2, count, planes, 2, devices, 2, half_slab, LANES)
    lower = spread[:, :, :, 0].reshape(2, count, planes, devices, slab_cells, LANES)
    lane = jnp.arange(LANES) < HALF
    higher = jnp.where(lane, spread[:, :, :, 1, :, 0], spread[:, :, :, 1, :, 1])
    blocks = jnp.concatenate([lower, higher], axis=4).transpose(3, 2, 0, 1, 4, 5)
    blocks, gathered = exchange(blocks, 0, alive, packed)
    gathered = gathered[:, : listed[0], : listed[1]].reshape(-1, listed[1])
    blocks = blocks.reshape(stored_planes, 2, count, rows, LANES)
    parcel = blocks.transpose(1, 2, 0, 3, 4)
    speed_one = parcel[:, 0]
    speed_two = parcel[:, 1]
    speed_three = parcel[:, 2]
    slope_two = parcel[:, 3]
    slope_three = parcel[:, 4]
    spin = jnp.stack(
        [
            rotate_quarter(column_waves * speed_three - third_waves * speed_two),
            rotate_quarter(third_waves * speed_one) - slope_three,
            slope_two - rotate_quarter(column_waves * speed_one),
        ],
        axis=1,
    )
    parcel = jnp.concatenate([parcel[:, :3], spin], axis=1)
    along_third = jnp.einsum("rfcnb,rcqz->qfznb", parcel, table_third, precision=PRECISE)
    physical = jnp.einsum(
        "rfznb,rby->fzny", along_third[..., :slab_cells, :], table_lower, precision=PRECISE
    )
    physical = physical + jnp.einsum(
        "rfznb,rbhy->fzhny", along_third[..., slab_cells:, :], table_upper, precision=PRECISE
    ).reshape(physical.shape)
    velocity = physical[:3]
    vorticity = physical[3:]
    crossed = jnp.stack(
        [
            velocity[1] * vorticity[2] - velocity[2] * vorticity[1],
            velocity[2] * vorticity[0] - velocity[0] * vorticity[2],
            velocity[0] * vorticity[1] - velocity[1] * vorticity[0],
        ]
    )
    halves = crossed.reshape(3, depth_cells, 2, half_slab, NY)
    spectral_second = jnp.concatenate(
        [
            jnp.einsum("czny,rby->rcznb", crossed, table_lower, precision=PRECISE),
            jnp.einsum("czhny,rbhy->rcznb", halves, table_upper, precision=PRECISE),
        ],
        axis=3,
    )
    terms = jnp.einsum("rcznb,qkrz->kqcnb", spectral_second, table_third, precision=PRECISE)
    terms = terms.reshape(devices, planes, 2, 3, rows, LANES)
    pencils = exchange(terms, 1, alive)[0].transpose(2, 3, 1, 0, 4, 5)
    low = pencils[..., :slab_cells, :].reshape(2, 3, planes, NX, LANES)
    high = pencils[..., slab_cells:, :]
    table_split = table_first.reshape(2, kept_first, 2, devices, 2, half_slab)
    spectral_low = jnp.einsum("rfkxn,qarx->qfkan", low, table_first, precision=PRECISE)
    spectral_high = jnp.einsum(
        "rfkdnl,qardhn->hqfkal", high, table_split, precision=PRECISE
    )
    spectral_high = spectral_high[0, ..., :HALF] + spectral_high[1, ..., HALF:]
    spectral = jnp.concatenate([spectral_low, spectral_high], axis=-1)
    spectral = jnp.pad(spectral, [(0, 0)] * 4 + [(0, kept_second - LANES - HALF)])
    first_range = jnp.arange(kept_first, dtype=jnp.int32)
    second_range = jnp.arange(kept_second, dtype=jnp.int32)
    plane_range = jnp.arange(planes, dtype=jnp.int32)
    numbers = gathered[:, :3].astype(jnp.int32)
    phases = gathered[:, 3]
    directions = gathered[:, 4:7]
    column_hit = (jnp.mod(numbers[:, 0], kept_first)[:, None] == first_range[None, :]).astype(
        jnp.float32
    )
    second_hit = (numbers[:, 1][:, None] == second_range[None, :]).astype(jnp.float32)
    plane_hit = (
        (jnp.mod(numbers[:, 2], stored_planes) - first_plane)[:, None] == plane_range[None, :]
    ).astype(jnp.float32)
    turning = 2.0 * math.pi / PH * phases
    values = jnp.stack(
        [directions.T * jnp.cos(turning)[None, :], directions.T * jnp.sin(turning)[None, :]]
    )
    placed = (
        values[:, :, None, None, :]
        * plane_hit.T[None, None, :, None, :]
        * column_hit.T[None, None, None, :, :]
    )
    forced = jnp.einsum("rckan,nb->rckab", placed, second_hit, precision=PRECISE)
    driving = spectral * retained + forced
    inner = wave_first * driving[:, 0] + wave_second * driving[:, 1] + wave_third * driving[:, 2]
    squared = wave_first * wave_first + wave_second * wave_second + wave_third * wave_third
    anchor = (
        (modes_first[None, :, None] == 0)
        & (modes_second[None, None, :] == 0)
        & (third_local[:, None, None] == 0)
    )
    share = inner / jnp.where(anchor, 1.0, squared)
    projected = driving - jnp.stack(
        [wave_first * share, wave_second * share, wave_third * share], axis=1
    )
    tendency = projected - VISCOSITY * squared * section
    return (base + SECTION_WEIGHT * tendency, accum + ACCUM_WEIGHT * tendency)


def solution(mesh):
    placed = (
        P(None, None, ("members", "row"), None, None),
        P(None, None, ("members", "row"), None, None),
        P(None, None, ("members", "row"), None, None),
        P("members"),
        P(("members", "row"), None),
        P(("members", "row")),
        P(("members", "row"), None),
    )
    return jax.shard_map(
        on_device,
        mesh=mesh,
        in_specs=placed,
        out_specs=(
            P(None, None, ("members", "row"), None, None),
            P(None, None, ("members", "row"), None, None),
        ),
        check_vma=False,
    )
```
